32 devices in a mesh: ctx: 8 (over z, x), head: 4 (over y, core).
Axes of the slice: x: 2, y: 2, z: 4, core: 2. Of those that a mesh axis runs over, the one named last changes fastest.
Arguments:
- query_nope: bfloat16 [32, 16384], P('ctx', 'head'), may hold values from -15 to 15
- query_rope: bfloat16 [32, 8192], P('ctx', 'head'), may hold values from -8 to 8
- cache_latent: bfloat16 [512, 128, 512], P('ctx'), may hold values from -6 to 6
- cache_rope: bfloat16 [512, 8192], P('ctx'), may hold values from -8 to 8
- key_up: bfloat16 [128, 128, 512], P('head'), may hold values from -0.25 to 0.25
- value_up: bfloat16 [128, 512, 128], P('head'), may hold values from -0.25 to 0.25
- lengths: int32 [16], replicated, may hold values from 1024 to 4096, as said below
- block_owner: int32 [512], P('ctx'), may hold values from -1 to 15, as said below
- block_number: int32 [512], P('ctx'), may hold values from 0 to 31, as said below
Outputs:
- attended: bfloat16 [32, 16384], P('ctx', 'head')
The draws below stay inside these ranges and needn't reach their ends.
Inputs may be any that keep to these rules, and one draw needn't show every extreme that they name: `lengths`: at least one sequence has exactly 4096 positions. A slot with block_owner -1 holds nothing. Sequence b owns exactly ceil(lengths[b] / 128) slots. The slots of sequence b carry block_number 0 to ceil(lengths[b] / 128) - 1, each once; empty slots carry 0.
All inputs are finite; a program needn't handle non-finite values.
Results may differ from the reference program's by a relative error of at most 0.023.
Values may be sent and summed in bfloat16 or wider, within the bound.
A program may use at most 128 MiB of HBM per device.

```python
import math
import jax
import jax.numpy as jnp
from jax import lax

H = 128
NOPE = 128
ROPE = 64
KV_LAT = 512
V_HEAD = 128
SEQS = 16
QT = 2
BLK = 128
NB_DEV = 64
POOL = 512
ROWS = 32
MAX_LEN = 4096


def pool_layout(key):
    folded = jax.random.fold_in(key, 53)
    splits = jax.random.split(folded, 4)
    shortest = max(QT, MAX_LEN // 4)
    lengths = jax.random.randint(splits[0], (SEQS,), shortest, MAX_LEN + 1, dtype=jnp.int32)
    longest = jax.random.randint(splits[1], (), 0, SEQS, dtype=jnp.int32)
    lengths = jnp.where(jnp.arange(SEQS, dtype=jnp.int32) == longest, MAX_LEN, lengths).astype(jnp.int32)
    needed = (lengths + BLK - 1) // BLK
    block_ends = jnp.cumsum(needed).astype(jnp.int32)
    block_starts = block_ends - needed
    device_count = POOL // NB_DEV
    levels = jax.random.randint(splits[2], (device_count,), 0, 3, dtype=jnp.int32)
    jitter = jax.random.randint(splits[3], (POOL,), 0, 65536, dtype=jnp.int32)
    priority = jnp.repeat(levels, NB_DEV) * 32768 + jitter
    ordering = jnp.argsort(priority, stable=True).astype(jnp.int32)
    ranking = jnp.zeros((POOL,), jnp.int32).at[ordering].set(jnp.arange(POOL, dtype=jnp.int32))
    holder = jnp.sum((ranking[:, None] >= block_ends[None, :]).astype(jnp.int32), axis=1)
    occupied = holder < SEQS
    holder_safe = jnp.minimum(holder, SEQS - 1)
    owners = jnp.where(occupied, holder, -1).astype(jnp.int32)
    numbers = jnp.where(occupied, ranking - block_starts[holder_safe], 0).astype(jnp.int32)
    return (lengths, owners, numbers)


def draw_lengths(key, part):
    return pool_layout(key)[0]


def draw_block_owner(key, part):
    return pool_layout(key)[1]


def draw_block_number(key, part):
    return pool_layout(key)[2]


def draw_query_rope(key, part):
    drawn_key = jax.random.fold_in(key, 31)
    values = jnp.clip(jax.random.normal(drawn_key, (ROWS, H * ROPE), jnp.float32), -8.0, 8.0)
    return values.astype(jnp.bfloat16)


def draw_cache_rope(key, part):
    drawn_key = jax.random.fold_in(key, 41)
    values = jnp.clip(jax.random.normal(drawn_key, (POOL, BLK * ROPE), jnp.float32), -8.0, 8.0)
    return values.astype(jnp.bfloat16)


def block_scale(rng, shape, pieces, least, top_value):
    def one(position, blocks):
        draws = jax.random.uniform(jax.random.fold_in(jax.random.fold_in(rng, 6), position), (blocks,), jnp.float32, least / len(pieces), top_value / len(pieces))
        return jnp.repeat(jnp.exp(draws), shape[position] // blocks).reshape((-1,) + (1,) * (len(shape) - position - 1))

    level = one(*pieces[0])
    for cut in pieces[1:]:
        level = level * one(*cut)
    return level


def noise(own_key, dims, scale, bound, shards=(), held_as=jnp.bfloat16):
    gain = block_scale(own_key, dims, shards, -0.22, 0.18) if shards else 1.0
    result = jax.random.normal(own_key, dims, jnp.float32) * scale * gain
    return jnp.minimum(jnp.maximum(result, -bound), bound).astype(held_as)


def setup_inputs(seed: int = 0) -> dict:
    key_list = jax.random.split(jax.random.key(seed), 10)
    return {
        "query_nope": noise(key_list[0], (ROWS, H * NOPE), 2.5, 15.0, ((0, 8), (1, 4))),
        "query_rope": draw_query_rope(jax.random.fold_in(key_list[9], 71), 0),
        "cache_latent": noise(key_list[2], (POOL, BLK, KV_LAT), 1.0, 6.0, ((0, 8),)),
        "cache_rope": draw_cache_rope(jax.random.fold_in(key_list[9], 71), 0),
        "key_up": noise(key_list[4], (H, NOPE, KV_LAT), KV_LAT ** -0.5, 0.25, ((0, 4),)),
        "value_up": noise(key_list[5], (H, KV_LAT, V_HEAD), KV_LAT ** -0.5, 0.25, ((0, 4),)),
        "lengths": draw_lengths(jax.random.fold_in(key_list[9], 71), 0),
        "block_owner": draw_block_owner(jax.random.fold_in(key_list[9], 71), 0),
        "block_number": draw_block_number(jax.random.fold_in(key_list[9], 71), 0),
    }


score_scale = (192.0 ** -0.5) * (1.0 + 0.1 * math.log(40.0)) ** 2
floor_value = -1.0e30


def reference(query_nope, query_rope, cache_latent, cache_rope, key_up, value_up, lengths, block_owner, block_number):
    query_three = query_nope.reshape(ROWS, H, NOPE).astype(jnp.float32)
    q_latent = jnp.einsum("rhn,hnc->rhc", query_three, key_up.astype(jnp.float32)).astype(jnp.bfloat16)
    q_latent = lax.optimization_barrier(q_latent)
    seq_query = q_latent.reshape(SEQS, QT * H, KV_LAT).astype(jnp.float32)
    seq_rope = query_rope.reshape(SEQS, QT * H, ROPE).astype(jnp.float32)
    per_step = math.gcd(POOL, 64)
    turn_count = POOL // per_step
    latent_sets = cache_latent.reshape(turn_count, per_step, BLK, KV_LAT)
    rope_sets = cache_rope.reshape(turn_count, per_step, BLK, ROPE)
    owner_sets = block_owner.reshape(turn_count, per_step)
    number_sets = block_number.reshape(turn_count, per_step)
    lag_ids = (QT - 1 - jnp.arange(QT)).astype(jnp.int32)
    seq_ids = jnp.arange(SEQS).astype(jnp.int32)
    slot_ids = jnp.arange(BLK).astype(jnp.int32)
    width_q = QT * H

    def advance(running, blockset):
        row_top, row_total, row_accum = running
        key_latent, rope_keys, owners, numbers = blockset
        owner_safe = jnp.clip(owners, 0, SEQS - 1)
        gathered = seq_query[owner_safe]
        gathered_rope = seq_rope[owner_safe]
        latent_real = key_latent.astype(jnp.float32)
        logits = jnp.einsum("gqc,gtc->gqt", gathered, latent_real, precision=lax.Precision.HIGHEST)
        logits = logits + jnp.einsum("gqd,gtd->gqt", gathered_rope, rope_keys.astype(jnp.float32), precision=lax.Precision.HIGHEST)
        logits = logits * score_scale
        positions = numbers[:, None] * BLK + slot_ids[None, :]
        limits = lengths[owner_safe][:, None] - lag_ids[None, :]
        visible = (owners[:, None, None] >= 0) & (positions[:, None, :] < limits[:, :, None])
        visible = jnp.broadcast_to(visible[:, :, None, :], (per_step, QT, H, BLK)).reshape(per_step, width_q, BLK)
        logits = jnp.where(visible, logits, floor_value)
        member = owners[:, None] == seq_ids[None, :]
        block_top = jnp.max(logits, axis=2)
        seq_top = jnp.max(jnp.where(member[:, :, None], block_top[:, None, :], floor_value), axis=0)
        new_top = jnp.maximum(row_top, seq_top)
        weight = jnp.where(visible, jnp.exp(logits - new_top[owner_safe][:, :, None]), 0.0)
        member_real = member.astype(jnp.float32)
        part_total = jnp.einsum("gb,gq->bq", member_real, jnp.sum(weight, axis=2), precision=lax.Precision.HIGHEST)
        weight_low = lax.optimization_barrier(weight.astype(jnp.bfloat16)).astype(jnp.float32)
        values = jnp.einsum("gqt,gtc->gqc", weight_low, latent_real, precision=lax.Precision.HIGHEST)
        part_accum = jnp.einsum("gb,gqc->bqc", member_real, values, precision=lax.Precision.HIGHEST)
        shrink = jnp.exp(row_top - new_top)
        return (new_top, row_total * shrink + part_total, row_accum * shrink[:, :, None] + part_accum), None

    starting = (jnp.full((SEQS, width_q), floor_value, jnp.float32), jnp.zeros((SEQS, width_q), jnp.float32), jnp.zeros((SEQS, width_q, KV_LAT), jnp.float32))
    running, unused = lax.scan(advance, starting, (latent_sets, rope_sets, owner_sets, number_sets))
    latent_out = (running[2] / running[1][:, :, None]).reshape(ROWS, H, KV_LAT)
    attended = jnp.einsum("rhc,hcv->rhv", latent_out, value_up.astype(jnp.float32), precision=lax.Precision.HIGHEST)
    return attended.astype(jnp.bfloat16).reshape(ROWS, H * V_HEAD)
```

```python
import functools
import math

import jax
import jax.numpy as jnp
from jax import lax
from jax.experimental import pallas as pl
from jax.experimental.pallas import tpu as pltpu
from jax.sharding import PartitionSpec as P

score_scale = 192.0 ** (-0.5) * (1.0 + 0.1 * math.log(40.0)) ** 2
floor_value = -1e30
LANES = 128
MESH = pl.DeviceIdType.MESH


def greet(count, me):
    barrier = pltpu.get_barrier_semaphore()
    for step in range(1, count):
        peer = lax.rem(me + step, count)
        pl.semaphore_signal(barrier, inc=1, device_id={"ctx": peer}, device_id_type=MESH)
    pl.semaphore_wait(barrier, count - 1)


def absorb_kernel(
    count, qn_ref, qr_ref, ku_hbm, q_ref, qn_all, qr_all, qn_wide, qr_wide, q_wide, ku,
    send_a, recv_a, send_b, recv_b, own_sem, ku_sem,
):
    me = lax.axis_index("ctx")
    heads = ku.shape[0]
    latent_tiles = ku.shape[2] // LANES
    row_part = qn_ref.shape[0]
    rows_all = row_part * count
    rope_width = qr_ref.shape[1] // heads
    weights = pltpu.make_async_copy(ku_hbm, ku, ku_sem)
    weights.start()
    own = [
        pltpu.make_async_copy(qn_ref, qn_all.at[me], own_sem.at[0]),
        pltpu.make_async_copy(qr_ref, qr_all.at[me], own_sem.at[1]),
    ]
    for copy in own:
        copy.start()
    greet(count, me)
    copies = []
    for step in range(1, count):
        peer = lax.rem(me + step, count)
        for src, dst, send_sem, recv_sem in (
            (qn_ref, qn_all, send_a, recv_a),
            (qr_ref, qr_all, send_b, recv_b),
        ):
            copy = pltpu.make_async_remote_copy(
                src_ref=src, dst_ref=dst.at[me], send_sem=send_sem.at[step],
                recv_sem=recv_sem.at[step], device_id={"ctx": peer}, device_id_type=MESH,
            )
            copy.start()
            copies.append(copy)
    for copy in own:
        copy.wait()
    for copy in copies:
        copy.wait()
    weights.wait()
    for source in range(count):
        rows = pl.ds(source * row_part, row_part)
        qn_wide[rows, :] = qn_all[source].astype(jnp.float32)
        qr_wide[rows, :] = qr_all[source].astype(jnp.float32)

    group = 4

    def one_group(turn, carry):
        for inner in range(group):
            head = turn * group + inner
            lanes = pl.ds(pl.multiple_of(head * LANES, LANES), LANES)
            query = qn_wide[:, lanes].astype(jnp.bfloat16)
            result = jnp.dot(query, ku[head], preferred_element_type=jnp.float32)
            for tile in range(latent_tiles):
                q_wide[tile, pl.ds(head, rows_all, stride=heads), :] = result[
                    :, tile * LANES : (tile + 1) * LANES
                ]
        return carry

    lax.fori_loop(0, heads // group, one_group, 0)
    low = lax.broadcasted_iota(jnp.int32, (rows_all, LANES), 1) < rope_width
    for pair in range(heads // 2):
        chunk = qr_wide[:, pair * LANES : (pair + 1) * LANES]
        turned = pltpu.roll(chunk, rope_width, 1)
        q_wide[latent_tiles, pl.ds(2 * pair, rows_all, stride=heads), :] = jnp.where(
            low, chunk, turned
        )
        q_wide[latent_tiles, pl.ds(2 * pair + 1, rows_all, stride=heads), :] = jnp.where(
            low, turned, chunk
        )
    for tile in range(latent_tiles + 1):
        q_ref[:, tile * LANES : (tile + 1) * LANES] = q_wide[tile].astype(jnp.bfloat16)


def attend_kernel(
    count, new_tokens, lengths, owners, numbers, q_ref, lat_hbm, rope_hbm, vu_hbm, out_ref,
    stat_ref, lat, rope, keys, scores, tops, totals, accum, values, vu, lat_sem, rope_sem, vu_sem,
):
    blocks, width, latent_width = lat.shape
    latent_tiles = latent_width // LANES
    heads = vu.shape[0]
    seq_rows = new_tokens * heads
    queries = q_ref.shape[0]
    rows_all = queries // heads
    dest_rows = queries // count
    sets = lat_sem.shape[0]
    per_set = blocks // sets
    rope_copy = pltpu.make_async_copy(rope_hbm, rope, rope_sem)
    rope_copy.start()

    def lat_copy(part):
        span = pl.ds(part * per_set, per_set)
        return pltpu.make_async_copy(lat_hbm.at[span], lat.at[span], lat_sem.at[part])

    for part in range(sets):
        lat_copy(part).start()
    vu_copy = pltpu.make_async_copy(vu_hbm, vu, vu_sem)
    vu_copy.start()
    tops[...] = jnp.full(tops.shape, floor_value, jnp.float32)
    totals[...] = jnp.zeros(totals.shape, jnp.float32)
    accum[...] = jnp.zeros(accum.shape, jnp.float32)
    rope_copy.wait()
    rope_width = rope.shape[1] // width
    low = lax.broadcasted_iota(jnp.int32, (blocks, LANES), 1) < rope_width

    def spread(pair, carry):
        lanes = pl.ds(pl.multiple_of(pair * LANES, LANES), LANES)
        chunk = rope[:, lanes].astype(jnp.float32)
        keys[pl.ds(2 * pair, blocks, stride=width), :] = jnp.where(low, chunk, 0.0)
        keys[pl.ds(2 * pair + 1, blocks, stride=width), :] = jnp.where(low, 0.0, chunk)
        return carry

    lax.fori_loop(0, width // 2, spread, 0, unroll=4)

    token = lax.broadcasted_iota(jnp.int32, (seq_rows, width), 0) // heads
    slot = lax.broadcasted_iota(jnp.int32, (seq_rows, width), 1)
    offset = slot - token
    contract_last = (((1,), (1,)), ((), ()))

    def score_one(block):
        owner = owners[block]
        safe = jnp.maximum(owner, 0)
        rows = pl.ds(pl.multiple_of(safe * seq_rows, seq_rows), seq_rows)
        low_key = keys[pl.ds(pl.multiple_of(block * width, width), width), :].astype(jnp.bfloat16)
        logits = lax.dot_general(
            q_ref[rows, :latent_width], lat[block], contract_last,
            preferred_element_type=jnp.float32,
        ) + lax.dot_general(
            q_ref[rows, latent_width:], low_key, contract_last, preferred_element_type=jnp.float32
        )
        limit = lengths[safe] - (new_tokens - 1) - numbers[block] * width
        limit = jnp.where(owner >= 0, limit, -width)
        logits = jnp.where(offset < limit, logits * score_scale, floor_value)
        return rows, logits

    def score_set(part, carry):
        lat_copy(part).wait()
        for inner in range(per_set):
            block = part * per_set + inner
            rows, logits = score_one(block)
            scores[block] = logits
            tops[rows, :] = jnp.maximum(tops[rows, :], logits)
        return carry

    lax.fori_loop(0, sets, score_set, 0)
    for row in range(0, queries, seq_rows):
        rows = pl.ds(row, seq_rows)
        top = jnp.max(tops[rows, :], axis=1, keepdims=True)
        tops[rows, :] = jnp.broadcast_to(jnp.maximum(top, 0.1 * floor_value), (seq_rows, LANES))

    def weigh_set(part, carry):
        for inner in range(per_set):
            block = part * per_set + inner
            safe = jnp.maximum(owners[block], 0)
            rows = pl.ds(pl.multiple_of(safe * seq_rows, seq_rows), seq_rows)
            weight = jnp.exp(scores[block] - tops[rows, :])
            totals[rows, :] += weight
            part_accum = jnp.dot(
                weight.astype(jnp.bfloat16), lat[block], preferred_element_type=jnp.float32
            )
            for tile in range(latent_tiles):
                accum[tile, rows, :] += part_accum[:, tile * LANES : (tile + 1) * LANES]
        return carry

    lax.fori_loop(0, sets, weigh_set, 0)
    vu_copy.wait()
    group = 4

    def lift(turn, carry):
        for inner in range(group):
            head = turn * group + inner
            picked = pl.ds(head, rows_all, stride=heads)
            result = jnp.zeros((rows_all, LANES), jnp.float32)
            whole = jnp.concatenate(
                [accum[tile, picked, :].astype(jnp.bfloat16) for tile in range(latent_tiles)],
                axis=1,
            )
            values[picked, :] = jnp.dot(whole, vu[head], preferred_element_type=jnp.float32)
        return carry

    lax.fori_loop(0, heads // group, lift, 0)
    for dest in range(count):
        rows = pl.ds(dest * dest_rows, dest_rows)
        total = jnp.sum(totals[rows, :], axis=1, keepdims=True)
        held = total > 0.0
        safe_total = jnp.where(held, total, 1.0)
        mass = jnp.where(held, tops[rows, :] + jnp.log(safe_total), floor_value)
        out_ref[dest] = (values[rows, :] * (1.0 / safe_total)).astype(jnp.bfloat16)
        stat_ref[dest] = jnp.transpose(mass)[: stat_ref.shape[1], :]


def merge_kernel(
    count, heads, out_ref, stat_ref, result_ref, outs, stats, merged,
    send_a, recv_a, send_b, recv_b, own_sem,
):
    me = lax.axis_index("ctx")
    row_part = result_ref.shape[0]
    own = [
        pltpu.make_async_copy(out_ref.at[me], outs.at[me], own_sem.at[0]),
        pltpu.make_async_copy(stat_ref.at[me], stats.at[me], own_sem.at[1]),
    ]
    for copy in own:
        copy.start()
    greet(count, me)
    copies = []
    for step in range(1, count):
        peer = lax.rem(me + step, count)
        for src, dst, send_sem, recv_sem in (
            (stat_ref, stats, send_b, recv_b),
            (out_ref, outs, send_a, recv_a),
        ):
            copy = pltpu.make_async_remote_copy(
                src_ref=src.at[peer], dst_ref=dst.at[me], send_sem=send_sem.at[step],
                recv_sem=recv_sem.at[step], device_id={"ctx": peer}, device_id_type=MESH,
            )
            copy.start()
            copies.append(copy)
    for copy in own:
        copy.wait()
    for copy in copies:
        copy.wait()
    columns = [jnp.transpose(stats[source]) for source in range(count)]
    top = functools.reduce(jnp.maximum, columns)
    parts = [jnp.exp(column - top) for column in columns]
    total = functools.reduce(jnp.add, parts)
    inverse = 1.0 / total
    sum_parts = None
    for source in range(count):
        piece = (parts[source] * inverse)[:, :1] * outs[source].astype(jnp.float32)
        sum_parts = piece if sum_parts is None else sum_parts + piece
    merged[...] = sum_parts
    for head in range(heads):
        result_ref[:, head * LANES : (head + 1) * LANES] = merged[
            pl.ds(head, row_part, stride=heads), :
        ].astype(jnp.bfloat16)


def per_device(
    query_nope, query_rope, cache_latent, cache_rope, key_up, value_up, lengths, block_owner,
    block_number,
):
    count = lax.axis_size("ctx")
    row_part = query_nope.shape[0]
    heads, nope_width, latent_width = key_up.shape
    value_width = value_up.shape[2]
    rows_all = row_part * count
    new_tokens = rows_all // lengths.shape[0]
    blocks, width, _ = cache_latent.shape
    queries = rows_all * heads
    q_width = latent_width + LANES
    latent_tiles = latent_width // LANES
    dest_rows = row_part * heads
    vmem = pl.BlockSpec(memory_space=pltpu.VMEM)
    smem = pl.BlockSpec(memory_space=pltpu.SMEM)
    hbm = pl.BlockSpec(memory_space=pl.ANY)
    dma = pltpu.SemaphoreType.DMA
    f32, bf16 = jnp.float32, jnp.bfloat16
    query = pl.pallas_call(
        functools.partial(absorb_kernel, count),
        name="absorb",
        out_shape=jax.ShapeDtypeStruct((queries, q_width), bf16),
        in_specs=[vmem, vmem, hbm],
        out_specs=vmem,
        scratch_shapes=[
            pltpu.VMEM((count,) + query_nope.shape, bf16),
            pltpu.VMEM((count,) + query_rope.shape, bf16),
            pltpu.VMEM((rows_all, query_nope.shape[1]), f32),
            pltpu.VMEM((rows_all, query_rope.shape[1]), f32),
            pltpu.VMEM((latent_tiles + 1, queries, LANES), f32),
            pltpu.VMEM(key_up.shape, bf16),
            dma((count,)), dma((count,)), dma((count,)), dma((count,)), dma((2,)), dma,
        ],
        compiler_params=pltpu.CompilerParams(
            collective_id=0, has_side_effects=True, vmem_limit_bytes=24 * 1024 * 1024
        ),
    )(query_nope, query_rope, key_up)
    sets = 8
    outs, stats = pl.pallas_call(
        functools.partial(attend_kernel, count, new_tokens),
        name="attend",
        out_shape=(
            jax.ShapeDtypeStruct((count, dest_rows, value_width), bf16),
            jax.ShapeDtypeStruct((count, 8, dest_rows), f32),
        ),
        in_specs=[smem, smem, smem, vmem, hbm, hbm, hbm],
        out_specs=(vmem, vmem),
        scratch_shapes=[
            pltpu.VMEM(cache_latent.shape, bf16),
            pltpu.VMEM(cache_rope.shape, bf16),
            pltpu.VMEM((blocks * width, LANES), f32),
            pltpu.VMEM((blocks, new_tokens * heads, width), f32),
            pltpu.VMEM((queries, LANES), f32),
            pltpu.VMEM((queries, LANES), f32),
            pltpu.VMEM((latent_tiles, queries, LANES), f32),
            pltpu.VMEM((queries, LANES), f32),
            pltpu.VMEM(value_up.shape, bf16),
            dma((sets,)), dma, dma,
        ],
        compiler_params=pltpu.CompilerParams(vmem_limit_bytes=48 * 1024 * 1024),
    )(lengths, block_owner, block_number, query, cache_latent, cache_rope, value_up)
    return pl.pallas_call(
        functools.partial(merge_kernel, count, heads),
        name="merge",
        out_shape=jax.ShapeDtypeStruct((row_part, heads * value_width), bf16),
        in_specs=[vmem, vmem],
        out_specs=vmem,
        scratch_shapes=[
            pltpu.VMEM((count, dest_rows, value_width), bf16),
            pltpu.VMEM((count, 8, dest_rows), f32),
            pltpu.VMEM((dest_rows, LANES), f32),
            dma((count,)), dma((count,)), dma((count,)), dma((count,)), dma((2,)),
        ],
        compiler_params=pltpu.CompilerParams(
            collective_id=1, has_side_effects=True, vmem_limit_bytes=16 * 1024 * 1024
        ),
    )(outs, stats)


def solution(mesh):
    return jax.shard_map(
        per_device,
        mesh=mesh,
        in_specs=(
            P("ctx", "head"),
            P("ctx", "head"),
            P("ctx", None, None),
            P("ctx", None),
            P("head", None, None),
            P("head", None, None),
            P(),
            P("ctx"),
            P("ctx"),
        ),
        out_specs=P("ctx", "head"),
        check_vma=False,
    )
```

```python
import functools
import math

import jax
import jax.numpy as jnp
from jax import lax
from jax.experimental import pallas as pl
from jax.experimental.pallas import tpu as pltpu
from jax.sharding import PartitionSpec as P

score_scale = 192.0 ** (-0.5) * (1.0 + 0.1 * math.log(40.0)) ** 2
floor_value = -1e30
LANES = 128
MESH = pl.DeviceIdType.MESH


def greet(count, me):
    barrier = pltpu.get_barrier_semaphore()
    for step in range(1, count):
        peer = lax.rem(me + step, count)
        pl.semaphore_signal(barrier, inc=1, device_id={"ctx": peer}, device_id_type=MESH)
    pl.semaphore_wait(barrier, count - 1)


def remote(src, dst, send_sem, recv_sem, peer):
    return pltpu.make_async_remote_copy(
        src_ref=src, dst_ref=dst, send_sem=send_sem, recv_sem=recv_sem,
        device_id={"ctx": peer}, device_id_type=MESH,
    )


def absorb_kernel(
    count, groups, qn_hbm, qr_hbm, ku_hbm, lat_hbm, rope_hbm, vu_hbm, q_ref, lat_a, lat_b,
    lat_c, lat_d, key_ref, vu_ref, qn_all, qr_all, qn_wide, qr_wide, q_wide, ku, rope, keys,
    send_z, recv_z, send_x, recv_x, own_sem, load_sem,
):
    me = lax.axis_index("ctx")
    outer = count // 2
    line, side = me // 2, lax.rem(me, 2)
    partner = me + 1 - 2 * side
    heads = ku.shape[0]
    latent_tiles = ku.shape[2] // LANES
    row_part = qn_hbm.shape[0]
    rows_all = row_part * count
    rope_width = qr_hbm.shape[1] // heads
    blocks = rope.shape[0]
    width = key_ref.shape[0] // blocks
    group_heads = heads // groups
    span = group_heads * LANES
    own = [
        pltpu.make_async_copy(
            qn_hbm.at[:, pl.ds(part * span, span)], qn_all.at[part, me], own_sem.at[part]
        )
        for part in range(groups)
    ] + [pltpu.make_async_copy(qr_hbm, qr_all.at[me], own_sem.at[groups])]
    lat_refs = (lat_a, lat_b, lat_c, lat_d)
    quarter = blocks // len(lat_refs)
    lat_parts = [
        (lat_hbm.at[pl.ds(place * quarter, quarter)], ref) for place, ref in enumerate(lat_refs)
    ]
    loads = [
        pltpu.make_async_copy(src, dst, load_sem.at[place])
        for place, (src, dst) in enumerate(
            [(rope_hbm, rope), (ku_hbm, ku)] + lat_parts + [(vu_hbm, vu_ref)]
        )
    ]
    for copy in own:
        copy.start()
    for copy in loads:
        copy.start()
    greet(count, me)

    def held(part, owner):
        return qr_all.at[owner] if part == groups else qn_all.at[part, owner]

    def along(part, step):
        peer = lax.rem(line + step, outer) * 2 + side
        return remote(
            held(part, me), held(part, me), send_z.at[part, step], recv_z.at[part, step], peer
        )

    def across(part, step):
        owner = lax.rem(line + outer - step, outer) * 2 + side
        return remote(
            held(part, owner), held(part, owner), send_x.at[part, step], recv_x.at[part, step],
            partner,
        )

    for part in range(groups + 1):
        own[part].wait()
        for step in range(1, outer):
            along(part, step).start()
        across(part, 0).start()

    def forward(part):
        for step in range(1, outer):
            along(part, step).wait_recv()
            across(part, step).start()

    loads[0].wait()
    low_key = lax.broadcasted_iota(jnp.int32, (blocks, LANES), 1) < rope_width

    def spread(pair, carry):
        lanes = pl.ds(pl.multiple_of(pair * LANES, LANES), LANES)
        chunk = rope[:, lanes].astype(jnp.float32)
        keys[pl.ds(2 * pair, blocks, stride=width), :] = jnp.where(low_key, chunk, 0.0)
        keys[pl.ds(2 * pair + 1, blocks, stride=width), :] = jnp.where(low_key, 0.0, chunk)
        return carry

    lax.fori_loop(0, width // 2, spread, 0, unroll=4)
    forward(0)

    def settle(block, carry):
        rows = pl.ds(pl.multiple_of(block * width, width), width)
        key_ref[rows, :] = keys[rows, :].astype(jnp.bfloat16)
        return carry

    lax.fori_loop(0, blocks, settle, 0, unroll=2)
    loads[1].wait()
    batch = 4
    for part in range(groups):
        forward(part + 1)
        for step in range(outer):
            across(part, step).wait_recv()
        for source in range(count):
            rows = pl.ds(source * row_part, row_part)
            qn_wide[rows, part * span : (part + 1) * span] = qn_all[part, source].astype(
                jnp.float32
            )

        def one_batch(turn, carry):
            for inner in range(batch):
                head = part * group_heads + turn * batch + inner
                lanes = pl.ds(pl.multiple_of(head * LANES, LANES), LANES)
                query = qn_wide[:, lanes].astype(jnp.bfloat16)
                result = jnp.dot(query, ku[head], preferred_element_type=jnp.float32)
                for tile in range(latent_tiles):
                    q_wide[tile, pl.ds(head, rows_all, stride=heads), :] = result[
                        :, tile * LANES : (tile + 1) * LANES
                    ]
            return carry

        lax.fori_loop(0, group_heads // batch, one_batch, 0)
    for step in range(outer):
        across(groups, step).wait_recv()
    for source in range(count):
        qr_wide[pl.ds(source * row_part, row_part), :] = qr_all[source].astype(jnp.float32)
    low = lax.broadcasted_iota(jnp.int32, (rows_all, LANES), 1) < rope_width
    for pair in range(heads // 2):
        chunk = qr_wide[:, pair * LANES : (pair + 1) * LANES]
        turned = pltpu.roll(chunk, rope_width, 1)
        q_wide[latent_tiles, pl.ds(2 * pair, rows_all, stride=heads), :] = jnp.where(
            low, chunk, turned
        )
        q_wide[latent_tiles, pl.ds(2 * pair + 1, rows_all, stride=heads), :] = jnp.where(
            low, turned, chunk
        )
    for tile in range(latent_tiles + 1):
        q_ref[:, tile * LANES : (tile + 1) * LANES] = q_wide[tile].astype(jnp.bfloat16)
    for part in range(groups + 1):
        across(part, 0).wait_send()
        for step in range(1, outer):
            along(part, step).wait_send()
            across(part, step).wait_send()
    for copy in loads[2:]:
        copy.wait()


def attend_kernel(
    count, heads, groups, new_tokens, lengths, owners, numbers, q_ref, lat_a, lat_b, lat_c, lat_d,
    keys, accum, inverse_ref, stat_ref, scores, tops, totals,
):
    lat_refs = (lat_a, lat_b, lat_c, lat_d)
    quarter, width, latent_width = lat_a.shape
    blocks = quarter * len(lat_refs)
    latent_tiles = latent_width // LANES
    seq_rows = new_tokens * heads
    queries = q_ref.shape[0]
    dest_rows = queries // count
    per_set = 8
    sets = quarter // per_set
    tops[...] = jnp.full(tops.shape, floor_value, jnp.float32)
    totals[...] = jnp.zeros(totals.shape, jnp.float32)
    accum[...] = jnp.zeros(accum.shape, jnp.float32)
    token = lax.broadcasted_iota(jnp.int32, (seq_rows, width), 0) // heads
    slot = lax.broadcasted_iota(jnp.int32, (seq_rows, width), 1)
    offset = slot - token
    contract_last = (((1,), (1,)), ((), ()))

    def score_one(block, latent):
        owner = owners[block]
        safe = jnp.maximum(owner, 0)
        rows = pl.ds(pl.multiple_of(safe * seq_rows, seq_rows), seq_rows)
        low_key = keys[pl.ds(pl.multiple_of(block * width, width), width), :]
        logits = lax.dot_general(
            q_ref[rows, :latent_width], latent, contract_last,
            preferred_element_type=jnp.float32,
        ) + lax.dot_general(
            q_ref[rows, latent_width:], low_key, contract_last, preferred_element_type=jnp.float32
        )
        limit = lengths[safe] - (new_tokens - 1) - numbers[block] * width
        limit = jnp.where(owner >= 0, limit, -width)
        logits = jnp.where(offset < limit, logits * score_scale, floor_value)
        return rows, logits

    for place, lat in enumerate(lat_refs):

        def score_set(part, carry):
            for inner in range(per_set):
                near = part * per_set + inner
                block = place * quarter + near
                rows, logits = score_one(block, lat[near])
                scores[block] = logits
                tops[rows, :] = jnp.maximum(tops[rows, :], logits)
            return carry

        lax.fori_loop(0, sets, score_set, 0)
    for row in range(0, queries, seq_rows):
        rows = pl.ds(row, seq_rows)
        top = jnp.max(tops[rows, :], axis=1, keepdims=True)
        tops[rows, :] = jnp.broadcast_to(jnp.maximum(top, 0.1 * floor_value), (seq_rows, LANES))

    for place, lat in enumerate(lat_refs):

        def weigh_set(part, carry):
            for inner in range(per_set):
                near = part * per_set + inner
                block = place * quarter + near
                safe = jnp.maximum(owners[block], 0)
                rows = pl.ds(pl.multiple_of(safe * seq_rows, seq_rows), seq_rows)
                weight = jnp.exp(scores[block] - tops[rows, :])
                totals[rows, :] += weight
                part_accum = jnp.dot(
                    weight.astype(jnp.bfloat16), lat[near], preferred_element_type=jnp.float32
                )
                for tile in range(latent_tiles):
                    accum[tile, rows, :] += part_accum[:, tile * LANES : (tile + 1) * LANES]
            return carry

        lax.fori_loop(0, sets, weigh_set, 0)
    group_heads = heads // groups
    for dest in range(count):
        rows = pl.ds(dest * dest_rows, dest_rows)
        total = jnp.sum(totals[rows, :], axis=1, keepdims=True)
        held = total > 0.0
        safe_total = jnp.where(held, total, 1.0)
        mass = jnp.where(held, tops[rows, :] + jnp.log(safe_total), floor_value)
        inverse_ref[rows, :] = jnp.broadcast_to(1.0 / safe_total, (dest_rows, LANES))
        ordered = jnp.concatenate(
            [
                mass[first : first + group_heads]
                for part in range(groups)
                for first in range(part * group_heads, dest_rows, heads)
            ],
            axis=0,
        )
        stat_ref[dest] = jnp.transpose(ordered)[:1, :]


def merge_kernel(
    count, groups, accum, inverse, stat_ref, vu, result_ref, values, sent, outs, stats, merged,
    send_a, recv_a, send_b, recv_b, own_sem,
):
    me = lax.axis_index("ctx")
    row_part = result_ref.shape[0]
    heads = vu.shape[0]
    latent_tiles = accum.shape[0]
    queries = accum.shape[1]
    rows_all = queries // heads
    group_heads = heads // groups
    group_rows = row_part * group_heads
    own_stat = pltpu.make_async_copy(stat_ref.at[me], stats.at[me], own_sem.at[groups])
    own_stat.start()
    greet(count, me)
    copies = [[] for part in range(groups + 1)]
    for step in range(1, count):
        peer = lax.rem(me + step, count)
        copy = remote(
            stat_ref.at[peer], stats.at[me], send_b.at[step], recv_b.at[step], peer
        )
        copy.start()
        copies[groups].append(copy)
    for part in range(groups):

        def lift(head, carry):
            picked = pl.ds(part * group_heads + head, rows_all, stride=heads)
            whole = jnp.concatenate(
                [accum[tile, picked, :].astype(jnp.bfloat16) for tile in range(latent_tiles)],
                axis=1,
            )
            lifted = jnp.dot(
                whole, vu[part * group_heads + head], preferred_element_type=jnp.float32
            )
            values[pl.ds(head, rows_all, stride=group_heads), :] = lifted * inverse[picked, :]
            return carry

        lax.fori_loop(0, group_heads, lift, 0, unroll=4)
        for dest in range(count):
            rows = pl.ds(dest * group_rows, group_rows)
            sent[part, dest] = values[rows, :].astype(jnp.bfloat16)
        own_part = pltpu.make_async_copy(
            sent.at[part, me], outs.at[part, me], own_sem.at[part]
        )
        own_part.start()
        copies[part].append(own_part)
        for step in range(1, count):
            peer = lax.rem(me + step, count)
            copy = remote(
                sent.at[part, peer], outs.at[part, me], send_a.at[part, step],
                recv_a.at[part, step], peer,
            )
            copy.start()
            copies[part].append(copy)
    own_stat.wait()
    for copy in copies[groups]:
        copy.wait()
    mass = jnp.transpose(stats[:, 0, :])
    share = jnp.exp(mass - jnp.max(mass, axis=1, keepdims=True))
    share = share * (1.0 / jnp.sum(share, axis=1, keepdims=True))
    for part in range(groups):
        for copy in copies[part]:
            copy.wait()
        total = None
        for source in range(count):
            piece = share[
                part * group_rows : (part + 1) * group_rows, source : source + 1
            ] * outs[part, source].astype(jnp.float32)
            total = piece if total is None else total + piece
        merged[...] = total
        for head in range(group_heads):
            first = (part * group_heads + head) * LANES
            result_ref[:, first : first + LANES] = merged[
                pl.ds(head, row_part, stride=group_heads), :
            ].astype(jnp.bfloat16)


def per_device(
    query_nope, query_rope, cache_latent, cache_rope, key_up, value_up, lengths, block_owner,
    block_number,
):
    count = lax.axis_size("ctx")
    row_part = query_nope.shape[0]
    heads, nope_width, latent_width = key_up.shape
    value_width = value_up.shape[2]
    rows_all = row_part * count
    new_tokens = rows_all // lengths.shape[0]
    blocks, width, _ = cache_latent.shape
    queries = rows_all * heads
    q_width = latent_width + LANES
    latent_tiles = latent_width // LANES
    dest_rows = row_part * heads
    groups = max(1, heads // count)
    group_heads = heads // groups
    outer = count // 2
    vmem = pl.BlockSpec(memory_space=pltpu.VMEM)
    smem = pl.BlockSpec(memory_space=pltpu.SMEM)
    hbm = pl.BlockSpec(memory_space=pltpu.HBM)
    dma = pltpu.SemaphoreType.DMA
    f32, bf16 = jnp.float32, jnp.bfloat16
    mib = 1024 * 1024
    quarter_shape = (blocks // 4,) + cache_latent.shape[1:]
    query, *latents, keys, lifts = pl.pallas_call(
        functools.partial(absorb_kernel, count, groups),
        name="absorb",
        out_shape=(
            jax.ShapeDtypeStruct((queries, q_width), bf16),
            *[jax.ShapeDtypeStruct(quarter_shape, bf16)] * 4,
            jax.ShapeDtypeStruct((blocks * width, LANES), bf16),
            jax.ShapeDtypeStruct(value_up.shape, bf16),
        ),
        in_specs=[hbm] * 6,
        out_specs=(vmem,) * 7,
        scratch_shapes=[
            pltpu.VMEM((groups, count, row_part, group_heads * nope_width), bf16),
            pltpu.VMEM((count,) + query_rope.shape, bf16),
            pltpu.VMEM((rows_all, query_nope.shape[1]), f32),
            pltpu.VMEM((rows_all, query_rope.shape[1]), f32),
            pltpu.VMEM((latent_tiles + 1, queries, LANES), f32),
            pltpu.VMEM(key_up.shape, bf16),
            pltpu.VMEM(cache_rope.shape, bf16),
            pltpu.VMEM((blocks * width, LANES), f32),
            dma((groups + 1, outer)), dma((groups + 1, outer)),
            dma((groups + 1, outer)), dma((groups + 1, outer)),
            dma((groups + 1,)), dma((7,)),
        ],
        compiler_params=pltpu.CompilerParams(
            collective_id=0, has_side_effects=True, vmem_limit_bytes=38_500_000
        ),
    )(query_nope, query_rope, key_up, cache_latent, cache_rope, value_up)
    accum, inverse, stats = pl.pallas_call(
        functools.partial(attend_kernel, count, heads, groups, new_tokens),
        name="attend",
        out_shape=(
            jax.ShapeDtypeStruct((latent_tiles, queries, LANES), f32),
            jax.ShapeDtypeStruct((queries, LANES), f32),
            jax.ShapeDtypeStruct((count, 1, dest_rows), f32),
        ),
        in_specs=[smem] * 3 + [vmem] * 6,
        out_specs=(vmem,) * 3,
        scratch_shapes=[
            pltpu.VMEM((blocks, new_tokens * heads, width), f32),
            pltpu.VMEM((queries, LANES), f32),
            pltpu.VMEM((queries, LANES), f32),
        ],
        compiler_params=pltpu.CompilerParams(vmem_limit_bytes=24 * mib),
    )(lengths, block_owner, block_number, query, *latents, keys)
    return pl.pallas_call(
        functools.partial(merge_kernel, count, groups),
        name="merge",
        out_shape=jax.ShapeDtypeStruct((row_part, heads * value_width), bf16),
        in_specs=[vmem] * 4,
        out_specs=vmem,
        scratch_shapes=[
            pltpu.VMEM((rows_all * group_heads, LANES), f32),
            pltpu.VMEM((groups, count, row_part * group_heads, value_width), bf16),
            pltpu.VMEM((groups, count, row_part * group_heads, value_width), bf16),
            pltpu.VMEM((count, 1, dest_rows), f32),
            pltpu.VMEM((row_part * group_heads, LANES), f32),
            dma((groups, count)), dma((groups, count)), dma((count,)), dma((count,)),
            dma((groups + 1,)),
        ],
        compiler_params=pltpu.CompilerParams(
            collective_id=1, has_side_effects=True, vmem_limit_bytes=16 * mib
        ),
    )(accum, inverse, stats, lifts)


def solution(mesh):
    return jax.shard_map(
        per_device,
        mesh=mesh,
        in_specs=(
            P("ctx", "head"),
            P("ctx", "head"),
            P("ctx", None, None),
            P("ctx", None),
            P("head", None, None),
            P("head", None, None),
            P(),
            P("ctx"),
            P("ctx"),
        ),
        out_specs=P("ctx", "head"),
        check_vma=False,
    )
```

```python
import functools
import math

import jax
import jax.numpy as jnp
from jax import lax
from jax.experimental import pallas as pl
from jax.experimental.pallas import tpu as pltpu
from jax.sharding import PartitionSpec as P

score_scale = 192.0 ** (-0.5) * (1.0 + 0.1 * math.log(40.0)) ** 2
floor_value = -1e30
LANES = 128
MESH = pl.DeviceIdType.MESH


def greet(count, me):
    barrier = pltpu.get_barrier_semaphore()
    for step in range(1, count):
        peer = lax.rem(me + step, count)
        pl.semaphore_signal(barrier, inc=1, device_id={"ctx": peer}, device_id_type=MESH)
    pl.semaphore_wait(barrier, count - 1)


def remote(src, dst, send_sem, recv_sem, peer):
    return pltpu.make_async_remote_copy(
        src_ref=src, dst_ref=dst, send_sem=send_sem, recv_sem=recv_sem,
        device_id={"ctx": peer}, device_id_type=MESH,
    )


def absorb_kernel(
    count, groups, qn_hbm, qr_hbm, ku_hbm, lat_hbm, rope_hbm, vu_hbm, q_ref, lat_a, lat_b,
    lat_c, lat_d, key_ref, vu_ref, qn_all, qr_all, qn_wide, qr_wide, q_wide, ku, rope, keys,
    send_z, recv_z, own_sem, load_sem,
):
    me = lax.axis_index("ctx")
    heads = ku.shape[0]
    latent_tiles = ku.shape[2] // LANES
    row_part = qn_hbm.shape[0]
    rows_all = row_part * count
    rope_width = qr_hbm.shape[1] // heads
    blocks = rope.shape[0]
    width = key_ref.shape[0] // blocks
    group_heads = heads // groups
    span = group_heads * LANES
    own = [
        pltpu.make_async_copy(
            qn_hbm.at[:, pl.ds(part * span, span)], qn_all.at[part, me], own_sem.at[part]
        )
        for part in range(groups)
    ] + [pltpu.make_async_copy(qr_hbm, qr_all.at[me], own_sem.at[groups])]
    lat_refs = (lat_a, lat_b, lat_c, lat_d)
    quarter = blocks // len(lat_refs)
    lat_parts = [
        (lat_hbm.at[pl.ds(place * quarter, quarter)], ref) for place, ref in enumerate(lat_refs)
    ]
    loads = [
        pltpu.make_async_copy(src, dst, load_sem.at[place])
        for place, (src, dst) in enumerate(
            [(rope_hbm, rope), (ku_hbm, ku)] + lat_parts + [(vu_hbm, vu_ref)]
        )
    ]
    for copy in own:
        copy.start()
    for copy in loads:
        copy.start()
    greet(count, me)

    def held(part, owner):
        return qr_all.at[owner] if part == groups else qn_all.at[part, owner]

    def direct(part, step):
        return remote(
            held(part, me), held(part, me), send_z.at[part, step], recv_z.at[part, step],
            lax.rem(me + step, count),
        )

    for part in range(groups + 1):
        own[part].wait()
        for step in range(1, count):
            direct(part, step).start()

    loads[0].wait()
    low_key = lax.broadcasted_iota(jnp.int32, (blocks, LANES), 1) < rope_width

    def spread(pair, carry):
        lanes = pl.ds(pl.multiple_of(pair * LANES, LANES), LANES)
        chunk = rope[:, lanes].astype(jnp.float32)
        keys[pl.ds(2 * pair, blocks, stride=width), :] = jnp.where(low_key, chunk, 0.0)
        keys[pl.ds(2 * pair + 1, blocks, stride=width), :] = jnp.where(low_key, 0.0, chunk)
        return carry

    lax.fori_loop(0, width // 2, spread, 0, unroll=4)

    def settle(block, carry):
        rows = pl.ds(pl.multiple_of(block * width, width), width)
        key_ref[rows, :] = keys[rows, :].astype(jnp.bfloat16)
        return carry

    lax.fori_loop(0, blocks, settle, 0, unroll=2)
    loads[1].wait()
    batch = 4
    for part in range(groups):
        for step in range(1, count):
            direct(part, step).wait_recv()
        for source in range(count):
            rows = pl.ds(source * row_part, row_part)
            qn_wide[rows, part * span : (part + 1) * span] = qn_all[part, source].astype(
                jnp.float32
            )

        def one_batch(turn, carry):
            for inner in range(batch):
                head = part * group_heads + turn * batch + inner
                lanes = pl.ds(pl.multiple_of(head * LANES, LANES), LANES)
                query = qn_wide[:, lanes].astype(jnp.bfloat16)
                result = jnp.dot(query, ku[head], preferred_element_type=jnp.float32)
                for tile in range(latent_tiles):
                    q_wide[tile, pl.ds(head, rows_all, stride=heads), :] = result[
                        :, tile * LANES : (tile + 1) * LANES
                    ]
            return carry

        lax.fori_loop(0, group_heads // batch, one_batch, 0)
    for step in range(1, count):
        direct(groups, step).wait_recv()
    for source in range(count):
        qr_wide[pl.ds(source * row_part, row_part), :] = qr_all[source].astype(jnp.float32)
    low = lax.broadcasted_iota(jnp.int32, (rows_all, LANES), 1) < rope_width
    for pair in range(heads // 2):
        chunk = qr_wide[:, pair * LANES : (pair + 1) * LANES]
        turned = pltpu.roll(chunk, rope_width, 1)
        q_wide[latent_tiles, pl.ds(2 * pair, rows_all, stride=heads), :] = jnp.where(
            low, chunk, turned
        )
        q_wide[latent_tiles, pl.ds(2 * pair + 1, rows_all, stride=heads), :] = jnp.where(
            low, turned, chunk
        )
    for tile in range(latent_tiles + 1):
        q_ref[:, tile * LANES : (tile + 1) * LANES] = q_wide[tile].astype(jnp.bfloat16)
    for part in range(groups + 1):
        for step in range(1, count):
            direct(part, step).wait_send()
    for copy in loads[2:]:
        copy.wait()


def attend_kernel(
    count, heads, groups, new_tokens, lengths, owners, numbers, q_ref, lat_a, lat_b, lat_c, lat_d,
    keys, accum, inverse_ref, stat_ref, scores, tops, totals,
):
    lat_refs = (lat_a, lat_b, lat_c, lat_d)
    quarter, width, latent_width = lat_a.shape
    blocks = quarter * len(lat_refs)
    latent_tiles = latent_width // LANES
    seq_rows = new_tokens * heads
    queries = q_ref.shape[0]
    dest_rows = queries // count
    per_set = 8
    sets = quarter // per_set
    tops[...] = jnp.full(tops.shape, floor_value, jnp.float32)
    totals[...] = jnp.zeros(totals.shape, jnp.float32)
    accum[...] = jnp.zeros(accum.shape, jnp.float32)
    token = lax.broadcasted_iota(jnp.int32, (seq_rows, width), 0) // heads
    slot = lax.broadcasted_iota(jnp.int32, (seq_rows, width), 1)
    offset = slot - token
    contract_last = (((1,), (1,)), ((), ()))

    def score_one(block, latent):
        owner = owners[block]
        safe = jnp.maximum(owner, 0)
        rows = pl.ds(pl.multiple_of(safe * seq_rows, seq_rows), seq_rows)
        low_key = keys[pl.ds(pl.multiple_of(block * width, width), width), :]
        logits = lax.dot_general(
            q_ref[rows, :latent_width], latent, contract_last,
            preferred_element_type=jnp.float32,
        ) + lax.dot_general(
            q_ref[rows, latent_width:], low_key, contract_last, preferred_element_type=jnp.float32
        )
        limit = lengths[safe] - (new_tokens - 1) - numbers[block] * width
        limit = jnp.where(owner >= 0, limit, -width)
        logits = jnp.where(offset < limit, logits * score_scale, floor_value)
        return rows, logits

    for place, lat in enumerate(lat_refs):

        def score_set(part, carry):
            for inner in range(per_set):
                near = part * per_set + inner
                block = place * quarter + near
                rows, logits = score_one(block, lat[near])
                scores[block] = logits
                tops[rows, :] = jnp.maximum(tops[rows, :], logits)
            return carry

        lax.fori_loop(0, sets, score_set, 0)
    for row in range(0, queries, seq_rows):
        rows = pl.ds(row, seq_rows)
        top = jnp.max(tops[rows, :], axis=1, keepdims=True)
        tops[rows, :] = jnp.broadcast_to(jnp.maximum(top, 0.1 * floor_value), (seq_rows, LANES))

    for place, lat in enumerate(lat_refs):

        def weigh_set(part, carry):
            for inner in range(per_set):
                near = part * per_set + inner
                block = place * quarter + near
                safe = jnp.maximum(owners[block], 0)
                rows = pl.ds(pl.multiple_of(safe * seq_rows, seq_rows), seq_rows)
                weight = jnp.exp(scores[block] - tops[rows, :])
                totals[rows, :] += weight
                part_accum = jnp.dot(
                    weight.astype(jnp.bfloat16), lat[near], preferred_element_type=jnp.float32
                )
                for tile in range(latent_tiles):
                    accum[tile, rows, :] += part_accum[:, tile * LANES : (tile + 1) * LANES]
            return carry

        lax.fori_loop(0, sets, weigh_set, 0)
    group_heads = heads // groups
    for dest in range(count):
        rows = pl.ds(dest * dest_rows, dest_rows)
        total = jnp.sum(totals[rows, :], axis=1, keepdims=True)
        held = total > 0.0
        safe_total = jnp.where(held, total, 1.0)
        mass = jnp.where(held, tops[rows, :] + jnp.log(safe_total), floor_value)
        inverse_ref[rows, :] = jnp.broadcast_to(1.0 / safe_total, (dest_rows, LANES))
        ordered = jnp.concatenate(
            [
                mass[first : first + group_heads]
                for part in range(groups)
                for first in range(part * group_heads, dest_rows, heads)
            ],
            axis=0,
        )
        stat_ref[dest] = jnp.transpose(ordered)[:1, :]


def merge_kernel(
    count, groups, accum, inverse, stat_ref, vu, result_ref, values, sent, outs, stats, merged,
    send_a, recv_a, send_b, recv_b, own_sem,
):
    me = lax.axis_index("ctx")
    row_part = result_ref.shape[0]
    heads = vu.shape[0]
    latent_tiles = accum.shape[0]
    queries = accum.shape[1]
    rows_all = queries // heads
    group_heads = heads // groups
    group_rows = row_part * group_heads
    own_stat = pltpu.make_async_copy(stat_ref.at[me], stats.at[me], own_sem.at[groups])
    own_stat.start()
    greet(count, me)
    copies = [[] for part in range(groups + 1)]
    for step in range(1, count):
        peer = lax.rem(me + step, count)
        copy = remote(
            stat_ref.at[peer], stats.at[me], send_b.at[step], recv_b.at[step], peer
        )
        copy.start()
        copies[groups].append(copy)
    for part in range(groups):

        def lift(head, carry):
            picked = pl.ds(part * group_heads + head, rows_all, stride=heads)
            whole = jnp.concatenate(
                [accum[tile, picked, :].astype(jnp.bfloat16) for tile in range(latent_tiles)],
                axis=1,
            )
            lifted = jnp.dot(
                whole, vu[part * group_heads + head], preferred_element_type=jnp.float32
            )
            values[pl.ds(head, rows_all, stride=group_heads), :] = lifted * inverse[picked, :]
            return carry

        lax.fori_loop(0, group_heads, lift, 0, unroll=4)
        for dest in range(count):
            rows = pl.ds(dest * group_rows, group_rows)
            sent[part, dest] = values[rows, :].astype(jnp.bfloat16)
        own_part = pltpu.make_async_copy(
            sent.at[part, me], outs.at[part, me], own_sem.at[part]
        )
        own_part.start()
        copies[part].append(own_part)
        for step in range(1, count):
            peer = lax.rem(me + step, count)
            copy = remote(
                sent.at[part, peer], outs.at[part, me], send_a.at[part, step],
                recv_a.at[part, step], peer,
            )
            copy.start()
            copies[part].append(copy)
    own_stat.wait()
    for copy in copies[groups]:
        copy.wait()
    mass = jnp.transpose(stats[:, 0, :])
    share = jnp.exp(mass - jnp.max(mass, axis=1, keepdims=True))
    share = share * (1.0 / jnp.sum(share, axis=1, keepdims=True))
    for part in range(groups):
        for copy in copies[part]:
            copy.wait()
        total = None
        for source in range(count):
            piece = share[
                part * group_rows : (part + 1) * group_rows, source : source + 1
            ] * outs[part, source].astype(jnp.float32)
            total = piece if total is None else total + piece
        merged[...] = total
        for head in range(group_heads):
            first = (part * group_heads + head) * LANES
            result_ref[:, first : first + LANES] = merged[
                pl.ds(head, row_part, stride=group_heads), :
            ].astype(jnp.bfloat16)


def per_device(
    query_nope, query_rope, cache_latent, cache_rope, key_up, value_up, lengths, block_owner,
    block_number,
):
    count = lax.axis_size("ctx")
    row_part = query_nope.shape[0]
    heads, nope_width, latent_width = key_up.shape
    value_width = value_up.shape[2]
    rows_all = row_part * count
    new_tokens = rows_all // lengths.shape[0]
    blocks, width, _ = cache_latent.shape
    queries = rows_all * heads
    q_width = latent_width + LANES
    latent_tiles = latent_width // LANES
    dest_rows = row_part * heads
    groups = max(1, heads // count)
    group_heads = heads // groups
    vmem = pl.BlockSpec(memory_space=pltpu.VMEM)
    smem = pl.BlockSpec(memory_space=pltpu.SMEM)
    hbm = pl.BlockSpec(memory_space=pltpu.HBM)
    dma = pltpu.SemaphoreType.DMA
    f32, bf16 = jnp.float32, jnp.bfloat16
    mib = 1024 * 1024
    quarter_shape = (blocks // 4,) + cache_latent.shape[1:]
    query, *latents, keys, lifts = pl.pallas_call(
        functools.partial(absorb_kernel, count, groups),
        name="absorb",
        out_shape=(
            jax.ShapeDtypeStruct((queries, q_width), bf16),
            *[jax.ShapeDtypeStruct(quarter_shape, bf16)] * 4,
            jax.ShapeDtypeStruct((blocks * width, LANES), bf16),
            jax.ShapeDtypeStruct(value_up.shape, bf16),
        ),
        in_specs=[hbm] * 6,
        out_specs=(vmem,) * 7,
        scratch_shapes=[
            pltpu.VMEM((groups, count, row_part, group_heads * nope_width), bf16),
            pltpu.VMEM((count,) + query_rope.shape, bf16),
            pltpu.VMEM((rows_all, query_nope.shape[1]), f32),
            pltpu.VMEM((rows_all, query_rope.shape[1]), f32),
            pltpu.VMEM((latent_tiles + 1, queries, LANES), f32),
            pltpu.VMEM(key_up.shape, bf16),
            pltpu.VMEM(cache_rope.shape, bf16),
            pltpu.VMEM((blocks * width, LANES), f32),
            dma((groups + 1, count)), dma((groups + 1, count)),
            dma((groups + 1,)), dma((7,)),
        ],
        compiler_params=pltpu.CompilerParams(
            collective_id=0, has_side_effects=True, vmem_limit_bytes=38_500_000
        ),
    )(query_nope, query_rope, key_up, cache_latent, cache_rope, value_up)
    accum, inverse, stats = pl.pallas_call(
        functools.partial(attend_kernel, count, heads, groups, new_tokens),
        name="attend",
        out_shape=(
            jax.ShapeDtypeStruct((latent_tiles, queries, LANES), f32),
            jax.ShapeDtypeStruct((queries, LANES), f32),
            jax.ShapeDtypeStruct((count, 1, dest_rows), f32),
        ),
        in_specs=[smem] * 3 + [vmem] * 6,
        out_specs=(vmem,) * 3,
        scratch_shapes=[
            pltpu.VMEM((blocks, new_tokens * heads, width), f32),
            pltpu.VMEM((queries, LANES), f32),
            pltpu.VMEM((queries, LANES), f32),
        ],
        compiler_params=pltpu.CompilerParams(vmem_limit_bytes=24 * mib),
    )(lengths, block_owner, block_number, query, *latents, keys)
    return pl.pallas_call(
        functools.partial(merge_kernel, count, groups),
        name="merge",
        out_shape=jax.ShapeDtypeStruct((row_part, heads * value_width), bf16),
        in_specs=[vmem] * 4,
        out_specs=vmem,
        scratch_shapes=[
            pltpu.VMEM((rows_all * group_heads, LANES), f32),
            pltpu.VMEM((groups, count, row_part * group_heads, value_width), bf16),
            pltpu.VMEM((groups, count, row_part * group_heads, value_width), bf16),
            pltpu.VMEM((count, 1, dest_rows), f32),
            pltpu.VMEM((row_part * group_heads, LANES), f32),
            dma((groups, count)), dma((groups, count)), dma((count,)), dma((count,)),
            dma((groups + 1,)),
        ],
        compiler_params=pltpu.CompilerParams(
            collective_id=1, has_side_effects=True, vmem_limit_bytes=16 * mib
        ),
    )(accum, inverse, stats, lifts)


def solution(mesh):
    return jax.shard_map(
        per_device,
        mesh=mesh,
        in_specs=(
            P("ctx", "head"),
            P("ctx", "head"),
            P("ctx", None, None),
            P("ctx", None),
            P("head", None, None),
            P("head", None, None),
            P(),
            P("ctx"),
            P("ctx"),
        ),
        out_specs=P("ctx", "head"),
        check_vma=False,
    )
```
